32 devices in a mesh: dp: 4 (over y, x), expert: 8 (over z, core).
Axes of the slice: x: 2, y: 2, z: 4, core: 2. Of those that a mesh axis runs over, the one named last changes fastest.
Arguments:
- tokens: bfloat16 [4096, 2048], P(('dp', 'expert')), may hold values from -6 to 6
- expert_ids: int32 [4096, 2], P(('dp', 'expert')), may hold values from 0 to 7, all different within a row; in each aligned block of 128 rows (0 to 127, 128 to 255, ...) at most 48 rows name the same one
- route_weights: float32 [4096, 2], P(('dp', 'expert')), may hold values from 0.1 to 1
- w_gate: bfloat16 [8, 2048, 384], P('expert', 'dp'), may hold values from -0.125 to 0.125
- w_up: bfloat16 [8, 2048, 384], P('expert', 'dp'), may hold values from -0.125 to 0.125
- w_down: bfloat16 [8, 2048, 384], P('expert', 'dp'), may hold values from -0.3125 to 0.3125
- grad_out: bfloat16 [4096, 2048], P(('dp', 'expert')), may hold values from -6 to 6
Outputs:
- layer_out: bfloat16 [4096, 2048], P(('dp', 'expert'))
- token_grad: bfloat16 [4096, 2048], P(('dp', 'expert'))
- route_grad: float32 [4096, 2], P(('dp', 'expert'))
- gate_grad: bfloat16 [8, 2048, 384], P('expert', 'dp')
- up_grad: bfloat16 [8, 2048, 384], P('expert', 'dp')
- down_grad: bfloat16 [8, 2048, 384], P('expert', 'dp')
The draws below stay inside these ranges and needn't reach their ends.
Inputs may be any that keep to these rules, and one draw needn't show every extreme that they name: `expert_ids`: each token names 2 different experts. Among the tokens of one device (aligned blocks of 128 tokens) no expert is named more than 48 times, and in some blocks one is named exactly 48 times.
All inputs are finite; a program needn't handle non-finite values.
Results may differ from the reference program's by a relative error of at most 0.0065.
Values may be sent and summed in bfloat16 or wider, within the bound.
A program may use at most 64 MiB of HBM per device.

```python
import math
import jax
import jax.numpy as jnp
import numpy as np
from jax import lax

D = 2048
FF = 384
TOP = 2
TOK_DEV = 128
EXPERTS = 8
TOKENS = 4096
CAP = 48
N_DP = 4
N_EXPERT = 8


def block_levels(stream_key, shape, cuts, low, high):
    level = 1.0
    for dim, blocks in cuts:
        steps = jax.random.uniform(jax.random.fold_in(jax.random.fold_in(stream_key, 6), dim), (blocks,), jnp.float32, low / len(cuts), high / len(cuts))
        level = level * jnp.repeat(jnp.exp(steps), shape[dim] // blocks).reshape((-1,) + (1,) * (len(shape) - 1 - dim))
    return level


def shared_out(key, own, number, rows, amount, top, limit, lean):
    sequence = jax.random.permutation(key, amount)
    crowded, common = load_shares(amount, rows * top, limit, lean, True), load_shares(amount, rows * top, limit, lean, False)
    places = jnp.arange(amount)

    def named(lengths, turn):
        used = int((lengths > 0).sum())
        fixed = max(1, used // 4)
        moved = fixed + (places - fixed + turn * (used - fixed)) % max(1, amount - fixed)
        return jnp.zeros((amount,), jnp.int32).at[sequence[jnp.where(places < fixed, places, moved)]].set(jnp.asarray(lengths, jnp.int32))

    lengths = jnp.where(number % 4 == 0, named(crowded, number // 4), named(common, number - number // 4 - 1))
    mixed = jax.random.permutation(jax.random.fold_in(own, 3), amount)
    giver, sink = mixed[0:amount // 2 * 2:2], mixed[1:amount // 2 * 2:2]
    margin = jnp.minimum(lengths[giver] - 1, limit - lengths[sink]) // 2
    margin = jnp.where((giver == sequence[0]) | (sink == sequence[0]) | (lengths[sink] == 0), 0, jnp.maximum(margin, 0))
    moved = jax.random.randint(jax.random.fold_in(own, 4), (amount // 2,), 0, 1 << 20) % (margin + 1)
    lengths = lengths.at[giver].add(-moved).at[sink].add(moved)
    labels = jnp.searchsorted(jnp.cumsum(lengths), jnp.arange(rows * top), side="right").astype(jnp.int32)
    listing = labels.reshape(top, rows).T
    listing = listing[jax.random.permutation(jax.random.fold_in(own, 1), rows)]
    turn = jax.random.randint(jax.random.fold_in(own, 2), (rows, 1), 0, top)
    return jnp.take_along_axis(listing, (jnp.arange(top)[None, :] + turn) % top, axis=1)


def load_shares(amount, total, reach, slope, full):
    loads = [(1 << 20) // math.isqrt(grade ** slope) + 1 for grade in range(1, amount + 1)]
    largest = reach if full else min(reach, max(-(-total // amount), total * loads[0] // sum(loads)))
    least = 1 if total - largest >= amount - 1 else 0
    counts, rest = [largest] + [least] * (amount - 1), total - largest - least * (amount - 1)
    while rest > 0:
        candidates = [i for i in range(1, amount) if counts[i] < largest] or [i for i in range(1, amount) if counts[i] < reach]
        pool, left = sum([loads[i] for i in candidates]), rest
        for i in candidates:
            addition = min(reach - counts[i], max(1, left * loads[i] // pool), rest)
            counts[i] = counts[i] + addition
            rest = rest - addition
    return np.array(counts)


def scatter_about(own_key, extent, width, most, shards=(), kind=jnp.bfloat16):
    drawn = width * jax.random.normal(own_key, extent, jnp.float32)
    if shards:
        drawn = drawn * block_levels(own_key, extent, shards, -0.22, 0.18)
    return jnp.clip(drawn, -most, most).astype(kind)


def setup_inputs(seed: int = 0) -> dict:
    splits = jax.random.split(jax.random.key(seed), 8)
    tokens = scatter_about(splits[0], (TOKENS, D), 1.0, 6.0, ((0, 32),))
    expert_ids_keys = jax.random.split(jax.random.fold_in(splits[1], 1), TOKENS // TOK_DEV)
    expert_ids_turns = jax.random.permutation(jax.random.fold_in(splits[1], 3), TOKENS // TOK_DEV)
    expert_ids = jax.vmap(lambda own, number: shared_out(jax.random.fold_in(splits[1], 2), own, number, TOK_DEV, EXPERTS, TOP, CAP, 2))(expert_ids_keys, expert_ids_turns).reshape((TOKENS, TOP))
    route_weights = jnp.clip(jnp.exp(math.log(1.0) - 2.3025851 * jax.random.uniform(splits[2], (TOKENS, TOP), jnp.float32) ** block_levels(splits[2], (TOKENS, TOP), ((0, 32),), -0.2, 0.2)), 0.1, 1.0)
    w_gate = scatter_about(splits[3], (EXPERTS, D, FF), D ** -0.5, 0.125, ((0, 8), (1, 4)))
    w_up = scatter_about(splits[4], (EXPERTS, D, FF), D ** -0.5, 0.125, ((0, 8), (1, 4)))
    w_down = scatter_about(splits[5], (EXPERTS, D, FF), FF ** -0.5, 0.3125, ((0, 8), (1, 4)))
    grad_out = scatter_about(splits[6], (TOKENS, D), 1.0, 6.0, ((0, 32),))
    return {"tokens": tokens, "expert_ids": expert_ids, "route_weights": route_weights, "w_gate": w_gate, "w_up": w_up, "w_down": w_down, "grad_out": grad_out}


def reference(tokens, expert_ids, route_weights, w_gate, w_up, w_down, grad_out):
    slots = TOKENS * TOP
    most_rows = N_DP * N_EXPERT * CAP
    flat_ids = expert_ids.reshape(-1)
    flat_weights = route_weights.reshape(-1)

    def one_expert(carry, expert):
        out_acc, grad_acc, route_acc = carry
        picked = jnp.nonzero(flat_ids == expert, size=most_rows, fill_value=slots)[0].astype(jnp.int32)
        valid = picked < slots
        slot = jnp.minimum(picked, slots - 1).astype(jnp.int32)
        token = (slot // TOP).astype(jnp.int32)
        live = valid.astype(jnp.float32)
        rows = jnp.where(valid[:, None], tokens[token], jnp.zeros((), jnp.bfloat16))
        weight = flat_weights[slot] * live
        cotan = grad_out[token].astype(jnp.float32)
        gate_w = w_gate[expert]
        up_w = w_up[expert]
        down_w = w_down[expert]
        gate = jnp.dot(rows, gate_w, preferred_element_type=jnp.float32)
        up = jnp.dot(rows, up_w, preferred_element_type=jnp.float32)
        sig = jax.nn.sigmoid(gate)
        hidden = (gate * sig * up).astype(jnp.bfloat16)
        expert_out = jnp.dot(hidden, down_w.T, preferred_element_type=jnp.float32).astype(jnp.bfloat16)
        out_grad = (weight[:, None] * cotan).astype(jnp.bfloat16)
        hidden_grad = jnp.dot(out_grad, down_w, preferred_element_type=jnp.float32)
        gate_term = (hidden_grad * up * sig * (1.0 + gate * (1.0 - sig))).astype(jnp.bfloat16)
        up_term = (hidden_grad * gate * sig).astype(jnp.bfloat16)
        slot_grad = (jnp.dot(gate_term, gate_w.T, preferred_element_type=jnp.float32)
                     + jnp.dot(up_term, up_w.T, preferred_element_type=jnp.float32)).astype(jnp.bfloat16)
        out_f = expert_out.astype(jnp.float32)
        out_acc = out_acc.at[token].add(weight[:, None] * out_f)
        grad_acc = grad_acc.at[token].add(slot_grad.astype(jnp.float32) * live[:, None])
        route_acc = route_acc.at[slot].add(jnp.sum(cotan * out_f, axis=1) * live)
        gate_g = jnp.dot(rows.T, gate_term, preferred_element_type=jnp.float32).astype(jnp.bfloat16)
        up_g = jnp.dot(rows.T, up_term, preferred_element_type=jnp.float32).astype(jnp.bfloat16)
        down_g = jnp.dot(out_grad.T, hidden, preferred_element_type=jnp.float32).astype(jnp.bfloat16)
        return (out_acc, grad_acc, route_acc), (gate_g, up_g, down_g)

    start = (jnp.zeros((TOKENS, D), jnp.float32), jnp.zeros((TOKENS, D), jnp.float32),
             jnp.zeros((slots,), jnp.float32))
    carry, grads = lax.scan(one_expert, start, jnp.arange(EXPERTS, dtype=jnp.int32))
    out_acc, grad_acc, route_acc = carry
    return (out_acc.astype(jnp.bfloat16), grad_acc.astype(jnp.bfloat16),
            route_acc.reshape(TOKENS, TOP), grads[0], grads[1], grads[2])
```

```python
import functools

import jax
import jax.numpy as jnp
from jax import lax
from jax.experimental import pallas as pl
from jax.experimental.pallas import tpu as pltpu
from jax.sharding import PartitionSpec as P

BF16 = jnp.bfloat16
F32 = jnp.float32
CORES = 2
VMEM_MAX = 60 * 1024 * 1024


def slot_table(expert_ids, experts, capacity):
    flat = expert_ids.reshape(-1)
    count = flat.shape[0]
    same = flat[:, None] == flat[None, :]
    earlier = lax.broadcasted_iota(jnp.int32, (count, count), 0) > lax.broadcasted_iota(
        jnp.int32, (count, count), 1
    )
    rank = jnp.sum((same & earlier).astype(jnp.int32), axis=1)
    target = flat * capacity + rank
    columns = lax.broadcasted_iota(jnp.int32, (count, experts * capacity), 1)
    return (target[:, None] == columns).astype(jnp.bfloat16)


def contract_last(left, right):
    return lax.dot_general(
        left, right, (((1,), (1,)), ((), ())), preferred_element_type=jnp.float32
    )


def contract_first(left, right):
    return lax.dot_general(
        left, right, (((0,), (0,)), ((), ())), preferred_element_type=jnp.float32
    )


def expert_forward(rows, gate_w, up_w, down_w):
    gate = jnp.dot(rows, gate_w, preferred_element_type=jnp.float32)
    up = jnp.dot(rows, up_w, preferred_element_type=jnp.float32)
    sig = jax.nn.sigmoid(gate)
    hidden = (gate * sig * up).astype(jnp.bfloat16)
    expert_out = contract_last(hidden, down_w).astype(jnp.bfloat16)
    return (expert_out, (gate, up, sig, hidden))


def expert_backward(out_grad, saved, gate_w, up_w, down_w):
    gate, up, sig, hidden = saved
    hidden_grad = jnp.dot(out_grad, down_w, preferred_element_type=jnp.float32)
    gate_term = (hidden_grad * up * sig * (1.0 + gate * (1.0 - sig))).astype(jnp.bfloat16)
    up_term = (hidden_grad * gate * sig).astype(jnp.bfloat16)
    slot_grad = (contract_last(gate_term, gate_w) + contract_last(up_term, up_w)).astype(
        jnp.bfloat16
    )
    return (slot_grad, gate_term, up_term)


def weight_grads(rows, out_grad, gate_term, up_term, hidden):
    part_rows, part_grad = (
        lax.all_to_all(rows, "dp", split_axis=1, concat_axis=0, tiled=True),
        lax.all_to_all(out_grad, "dp", split_axis=1, concat_axis=0, tiled=True),
    )
    all_gate, all_up, all_hidden = (
        lax.all_gather(gate_term, "dp", axis=0, tiled=True),
        lax.all_gather(up_term, "dp", axis=0, tiled=True),
        lax.all_gather(hidden, "dp", axis=0, tiled=True),
    )
    down_g = contract_first(part_grad, all_hidden).astype(jnp.bfloat16)
    gate_g = contract_first(part_rows, all_gate).astype(jnp.bfloat16)
    up_g = contract_first(part_rows, all_up).astype(jnp.bfloat16)
    return (gate_g, up_g, down_g)


def body(tokens, expert_ids, route_weights, w_gate, w_up, w_down, grad_out):
    local = w_gate.shape[0]
    groups = lax.axis_size("expert")
    experts = local * groups
    count = tokens.shape[0]
    top = expert_ids.shape[1]
    width = tokens.shape[1]
    capacity = max(2, (3 * count * top + 2 * experts - 1) // (2 * experts))
    table = slot_table(expert_ids, experts, capacity)
    per_token = jnp.sum(table.reshape(count, top, experts * capacity), axis=1)
    send_rows = jnp.dot(per_token.T, tokens, preferred_element_type=jnp.float32)
    send_rows = send_rows.astype(jnp.bfloat16).reshape(experts, capacity, width)
    weighted = (route_weights[:, :, None] * grad_out.astype(jnp.float32)[:, None, :]).astype(
        jnp.bfloat16
    )
    send_grad = jnp.dot(
        table.T, weighted.reshape(count * top, width), preferred_element_type=jnp.float32
    )
    send_grad = send_grad.astype(jnp.bfloat16).reshape(experts, capacity, width)
    full_gate, full_up, full_down = (
        lax.all_gather(w_gate, "dp", axis=1, tiled=True),
        lax.all_gather(w_up, "dp", axis=1, tiled=True),
        lax.all_gather(w_down, "dp", axis=1, tiled=True),
    )
    received = lax.all_to_all(send_rows, "expert", split_axis=0, concat_axis=0, tiled=True)
    shaped = received.reshape(groups, local, capacity, width)
    saves = []
    inputs = []
    slot_expert = 0
    rows = shaped[:, slot_expert].reshape(groups * capacity, width)
    expert_out, saved = expert_forward(
        rows, full_gate[slot_expert], full_up[slot_expert], full_down[slot_expert]
    )
    outs = expert_out.reshape(groups, 1, capacity, width)
    saves.append(saved)
    inputs.append(rows)
    expert_outs, saves, inputs = (outs.reshape(experts, capacity, width), saves, inputs)
    back_out = lax.all_to_all(expert_outs, "expert", split_axis=0, concat_axis=0, tiled=True)
    received_grad = lax.all_to_all(send_grad, "expert", split_axis=0, concat_axis=0, tiled=True)
    shaped = received_grad.reshape(groups, local, capacity, width)
    slot_expert = 0
    out_grad = shaped[:, slot_expert].reshape(groups * capacity, width)
    slot_grad, gate_term, up_term = expert_backward(
        out_grad,
        saves[slot_expert],
        full_gate[slot_expert],
        full_up[slot_expert],
        full_down[slot_expert],
    )
    grads_in = slot_grad.reshape(groups, 1, capacity, width)
    gate_g, up_g, down_g = weight_grads(
        inputs[slot_expert], out_grad, gate_term, up_term, saves[slot_expert][3]
    )
    gate_list = [gate_g]
    up_list = [up_g]
    down_list = [down_g]
    slot_grads = grads_in.reshape(experts, capacity, width)
    gate_grad = jnp.stack(gate_list)
    up_grad = jnp.stack(up_list)
    down_grad = jnp.stack(down_list)
    back_grad = lax.all_to_all(slot_grads, "expert", split_axis=0, concat_axis=0, tiled=True)
    out_slots = jnp.dot(
        table, back_out.reshape(experts * capacity, width), preferred_element_type=jnp.float32
    )
    out_slots = out_slots.reshape(count, top, width)
    layer_out = jnp.sum(route_weights[:, :, None] * out_slots, axis=1).astype(jnp.bfloat16)
    route_grad = jnp.sum(grad_out.astype(jnp.float32)[:, None, :] * out_slots, axis=2)
    grad_slots = jnp.dot(
        table, back_grad.reshape(experts * capacity, width), preferred_element_type=jnp.float32
    )
    token_grad = jnp.sum(grad_slots.reshape(count, top, width), axis=1).astype(jnp.bfloat16)
    return (layer_out, token_grad, route_grad, gate_grad, up_grad, down_grad)


def pad16(n):
    return (n + 15) // 16 * 16


def prefix_count(member):
    t = member.shape[1]
    before = lax.broadcasted_iota(jnp.int32, (t, t), 0) < lax.broadcasted_iota(jnp.int32, (t, t), 1)
    return jnp.sum(member[:, :, None] * before.astype(F32)[None], axis=1)


def route_tables(expert_ids, route_weights, groups):
    count, top = expert_ids.shape
    stages = groups // CORES
    chip = lax.axis_index("expert") // CORES
    lanes = lax.broadcasted_iota(jnp.int32, (count,), 0)
    experts = lax.broadcasted_iota(jnp.int32, (groups, count), 0)
    member = jnp.zeros((groups, count), F32)
    weight = jnp.zeros((groups, count), F32)
    for k in range(top):
        hit = (expert_ids[:, k][None, :] == experts).astype(F32)
        member = member + hit
        weight = weight + hit * route_weights[:, k][None, :]
    slot = jnp.where(member > 0, prefix_count(member), -1.0)

    def position(first):
        key = jnp.where(first, lanes, lanes + count)
        return jnp.sum((key[:, None] < key[None, :]).astype(F32), axis=0)

    pos_up = position(jnp.any(expert_ids // CORES == stages - 1, axis=1))
    pos_down = position(jnp.any(expert_ids // CORES == 0, axis=1))
    dest = lax.broadcasted_iota(jnp.int32, (groups, 1), 0) // CORES
    pos = jnp.where(dest >= chip, pos_up[None, :], pos_down[None, :])
    pick = (pos[:, None, :] == lanes.astype(F32)[None, :, None]).astype(F32)
    slot_rows = jnp.sum(pick * slot[:, None, :], axis=2)
    weight_rows = jnp.sum(pick * weight[:, None, :], axis=2)
    swap = lambda a: a.reshape(stages, CORES, count)[:, ::-1].reshape(groups, count)
    zero = jnp.zeros_like(slot)
    meta = jnp.stack(
        [slot_rows, weight_rows, swap(slot_rows), slot, swap(slot), zero, zero, zero], axis=1
    )
    order = jnp.stack([pos_up, pos_down] + [jnp.zeros_like(pos_up)] * 6, axis=0)
    return meta, order


def one_hot(row, height):
    rows = lax.broadcasted_iota(jnp.int32, (height, row.shape[1]), 0).astype(F32)
    return (rows == row).astype(F32)


def choose(index, values):
    result = jnp.int32(values[0])
    for i in range(1, len(values)):
        result = jnp.where(index == i, jnp.int32(values[i]), result)
    return result


def visit_order(chip, stages):
    near = [s for d in range(stages) for s in ((chip - d, chip + d) if d else (chip,))]
    return [s for s in near if 0 <= s < stages]


def moe_kernel(
    groups, ndp, cap, edge,
    tok_ref, grad_ref, meta_ref, order_ref, wg_ref, wu_ref, wd_ref,
    out_ref, tgrad_ref, route_ref, gg_ref, ug_ref, dg_ref,
    blocks, own_down, metas, xr, gr, ogr, wr, wfull, y, partner, ret_in, ret_down, ret_out,
    grad_send, grad_own, grad_recv, route_out, route_in,
    in_send, in_recv, meta_send, meta_recv, w_send, w_recv, pc_send, pc_recv,
    ret_send, ret_recv, retd_recv, route_send, route_recv, gr_send, gr_recv,
):
    stages = groups // CORES
    count, width = tok_ref.shape
    part, ff = wg_ref.shape
    me = lax.axis_index("expert")
    dp = lax.axis_index("dp")
    chip, core = me // CORES, me % CORES
    mate = chip * CORES + (1 - core)
    at_edge = (chip == 0) | (chip == stages - 1)
    pending = []

    def copy(src, dst, ssem, rsem, where):
        return pltpu.make_async_remote_copy(
            src_ref=src, dst_ref=dst, send_sem=ssem, recv_sem=rsem,
            device_id=where, device_id_type=pl.DeviceIdType.MESH,
        )

    def send(cond, *args):
        if cond is None:
            copy(*args).start()
        else:
            pl.when(cond)(lambda: copy(*args).start())
        pending.append((cond, args))

    def send_rows(cond, short, src, dst, ssem, rsem, where):
        if edge == count:
            send(cond, src, dst, ssem, rsem, where)
            return
        full = jnp.logical_not(short)
        if cond is not None:
            short, full = cond & short, cond & full
        cut = pl.ds(0, edge)
        send(full, src, dst, ssem, rsem, where)
        send(short, src.at[cut], dst.at[cut], ssem, rsem, where)

    def wait_rows(cond, short, dst, sem):
        def one(c, ref):
            pl.when(c)(lambda: copy(ref, ref, sem, sem, {"expert": mate}).wait_recv())

        if edge == count:
            one(cond, dst)
            return
        one(cond & jnp.logical_not(short), dst)
        one(cond & short, dst.at[pl.ds(0, edge)])

    yes = chip >= 0
    if edge < count:
        rest = pl.ds(edge, count - edge)
        empty = jnp.zeros((count - edge, width), BF16)
        for t in range(2):
            for s in range(stages):
                blocks[0, t, s, rest] = empty
                blocks[1, t, s, rest] = empty
                ret_in[t, s, rest] = empty
            ret_down[t, rest] = empty
    for t in range(2):
        @pl.when(chip == stages - 1)
        def _():
            ret_in[t, chip] = jnp.zeros((count, width), BF16)

        @pl.when(chip == 0)
        def _():
            ret_down[t] = jnp.zeros((count, width), BF16)

    up_hot = one_hot(order_ref[0:1, :], count)
    down_hot = one_hot(order_ref[1:2, :], count)
    for t, ref in enumerate((tok_ref, grad_ref)):
        value = ref[...]
        blocks[0, t, chip] = jnp.dot(up_hot.astype(BF16), value, preferred_element_type=F32).astype(BF16)
        own_down[t] = jnp.dot(down_hot.astype(BF16), value, preferred_element_type=F32).astype(BF16)
    metas[me] = meta_ref[me]

    barrier = pltpu.get_barrier_semaphore()
    for off in range(1, groups):
        pl.semaphore_signal(barrier, inc=1, device_id={"expert": (me + off) % groups},
                            device_id_type=pl.DeviceIdType.MESH)
    for off in range(1, ndp):
        pl.semaphore_signal(barrier, inc=1, device_id={"dp": (dp + off) % ndp},
                            device_id_type=pl.DeviceIdType.MESH)
    pl.semaphore_wait(barrier, groups + ndp - 2)

    for off in range(1, groups):
        other = (me + off) % groups
        send(None, meta_ref.at[other], metas.at[me], meta_send.at[off - 1], meta_recv.at[off - 1],
             {"expert": other})
    has_up, has_down = chip < stages - 1, chip > 0
    up_dev, down_dev = {"expert": me + CORES}, {"expert": me - CORES}
    for t in range(2):
        send_rows(has_up, chip + 1 == stages - 1, blocks.at[0, t, chip], blocks.at[0, t, chip],
                  in_send.at[t, 0, 0], in_recv.at[0, t, chip], up_dev)
        send_rows(has_down, chip - 1 == 0, own_down.at[t], blocks.at[0, t, chip],
                  in_send.at[t, 0, 1], in_recv.at[0, t, chip], down_dev)
        send(None, blocks.at[0, t, chip], blocks.at[1, t, chip],
             in_send.at[t, 0, 2], in_recv.at[1, t, chip], {"expert": mate})
    for i, ref in enumerate((wg_ref, wu_ref, wd_ref)):
        for off in range(1, ndp):
            send(None, ref, wfull.at[i, dp], w_send.at[i, off - 1], w_recv.at[i, off - 1],
                 {"dp": (dp + off) % ndp})
        wfull[i, dp] = ref[...]
    for off in range(1, groups):
        copy(meta_ref.at[0], metas.at[0], meta_send.at[off - 1], meta_recv.at[off - 1],
             {"expert": mate}).wait_recv()

    table = [visit_order(z, stages) for z in range(stages)]
    source = [choose(chip, [table[z][q] for z in range(stages)]) for q in range(stages)]

    def compact(q, r):
        s = source[q]
        origin = s * CORES + (core if r == 0 else 1 - core)
        tile = metas[origin]
        hot = one_hot(tile[0:1, :], cap)
        scale = jnp.sum(hot * tile[1:2, :], axis=1, keepdims=True)
        hot = hot.astype(BF16)
        rows = pl.ds((q * 2 + r) * cap, cap)
        xr[rows, :] = jnp.dot(hot, blocks[r, 0, s], preferred_element_type=F32).astype(BF16)
        g = jnp.dot(hot, blocks[r, 1, s], preferred_element_type=F32)
        gr[rows, :] = g.astype(BF16)
        ogr[rows, :] = (scale * g).astype(BF16)
        wr[rows, :] = jnp.broadcast_to(scale, (cap, 128))

    compact(0, 0)
    for q in range(stages):
        s = source[q]
        if q:
            rising = s < chip
            nxt = jnp.where(rising, chip + 1, chip - 1)
            more = (nxt >= 0) & (nxt < stages)
            for t in range(2):
                wait_rows(yes, at_edge, blocks.at[0, t, s], in_recv.at[0, t, s])
                send_rows(more, (nxt == 0) | (nxt == stages - 1), blocks.at[0, t, s],
                          blocks.at[0, t, s], in_send.at[t, q, 0], in_recv.at[0, t, s],
                          {"expert": nxt * CORES + core})
                send_rows(None, at_edge, blocks.at[0, t, s], blocks.at[1, t, s],
                          in_send.at[t, q, 2], in_recv.at[1, t, s], {"expert": mate})
            compact(q, 0)
        for t in range(2):
            if q:
                wait_rows(yes, at_edge, blocks.at[1, t, s], in_recv.at[1, t, s])
            else:
                wait_rows(yes, chip < 0, blocks.at[1, t, s], in_recv.at[1, t, s])
        compact(q, 1)

    for i in range(3):
        for off in range(1, ndp):
            copy(wfull.at[i, 0], wfull.at[i, 0], w_send.at[i, 0], w_recv.at[i, off - 1],
                 {"expert": mate}).wait_recv()

    def nt(a, b):
        return lax.dot_general(a, b, (((1,), (1,)), ((), ())), preferred_element_type=F32)

    def tn(a, b):
        return lax.dot_general(a, b, (((0,), (0,)), ((), ())), preferred_element_type=F32)

    def cut(j):
        return pl.ds(j * part, part)

    total = xr.shape[0]
    gate = jnp.zeros((total, ff), F32)
    up = jnp.zeros((total, ff), F32)
    hg = jnp.zeros((total, ff), F32)
    for j in range(ndp):
        gate += jnp.dot(xr[:, cut(j)], wfull[0, j], preferred_element_type=F32)
        up += jnp.dot(xr[:, cut(j)], wfull[1, j], preferred_element_type=F32)
        hg += jnp.dot(ogr[:, cut(j)], wfull[2, j], preferred_element_type=F32)
    sig = jax.nn.sigmoid(gate)
    hidden = (gate * sig * up).astype(BF16)
    gt = (hg * up * sig * (1.0 + gate * (1.0 - sig))).astype(BF16)
    ut = (hg * gate * sig).astype(BF16)
    scale = wr[:, 0:1]
    dots = jnp.zeros((total, 1), F32)
    for j in range(ndp):
        eo = nt(hidden, wfull[2, j]).astype(BF16).astype(F32)
        y[0, :, cut(j)] = (scale * eo).astype(BF16)
        dots += jnp.sum(gr[:, cut(j)].astype(F32) * eo, axis=1, keepdims=True)
        y[1, :, cut(j)] = (nt(gt, wfull[0, j]) + nt(ut, wfull[1, j])).astype(BF16)

    for q in reversed(range(stages)):
        for t in range(2):
            send(None, y.at[t, pl.ds((q * 2 + 1) * cap, cap)], partner.at[t, q],
                 pc_send.at[t, q], pc_recv.at[t, q], {"expert": mate})

    both = jnp.concatenate([gt, ut], axis=1)

    def weight_slice(off):
        j = (dp + off) % ndp
        cols = pl.ds(pl.multiple_of(j * part, part), part)
        gu = tn(xr[:, cols], both)
        return gu[:, :ff], gu[:, ff:], tn(ogr[:, cols], hidden)

    def weight_part(off):
        for i, value in enumerate(weight_slice(off)):
            grad_send[i, off - 1] = value.astype(BF16)
        for i in range(3):
            send(None, grad_send.at[i, off - 1], grad_recv.at[i, off - 1], gr_send.at[i, off - 1],
                 gr_recv.at[i, off - 1], {"dp": (dp + off) % ndp})

    def expand(q, t, row_own, row_mate):
        tile = metas[source[q] * CORES + core]
        own = one_hot(tile[row_own:row_own + 1, :], cap).astype(BF16)
        other = one_hot(tile[row_mate:row_mate + 1, :], cap).astype(BF16)
        return tn(own, y[t, pl.ds(q * 2 * cap, cap), :]) + tn(other, partner[t, q])

    def give_back(q):
        s = source[q]
        rising = s > chip
        nxt = jnp.where(rising, chip + 1, chip - 1)
        back = jnp.where(rising, chip - 1, chip + 1)
        fed = (back >= 0) & (back < stages)
        where = {"expert": nxt * CORES + core}
        for t in range(2):
            copy(partner.at[t, q], partner.at[t, q], pc_send.at[t, q], pc_recv.at[t, q],
                 {"expert": mate}).wait_recv()
            value = expand(q, t, 0, 2)
            wait_rows(fed, (back == 0) | (back == stages - 1), ret_in.at[t, s], ret_recv.at[t, s])

            @pl.when(fed)
            def _():
                ret_out[t, q] = (value + ret_in[t, s].astype(F32)).astype(BF16)

            @pl.when(jnp.logical_not(fed))
            def _():
                ret_out[t, q] = value.astype(BF16)

            last_up = rising & (nxt == s)
            send_rows(last_up, at_edge, ret_out.at[t, q], ret_down.at[t], ret_send.at[t, q],
                      retd_recv.at[t], where)
            send_rows(jnp.logical_not(last_up), at_edge, ret_out.at[t, q], ret_in.at[t, s],
                      ret_send.at[t, q], ret_recv.at[t, s], where)

    for off in range(1, ndp):
        q = stages - off
        if q >= 1:
            give_back(q)
        weight_part(off)
    for q in reversed(range(1, stages - ndp + 1)):
        give_back(q)

    for q in range(stages):
        for r in range(2):
            origin = source[q] * CORES + (core if r == 0 else 1 - core)
            hot = one_hot(metas[origin][3:4, :], cap)
            part_dots = dots[(q * 2 + r) * cap:(q * 2 + r + 1) * cap, :]
            line = jnp.sum(hot * part_dots, axis=0, keepdims=True)
            route_out[origin] = jnp.broadcast_to(line, (8, count))
    for off in range(1, groups):
        other = (me + off) % groups
        send(None, route_out.at[other], route_in.at[me], route_send.at[off - 1],
             route_recv.at[off - 1], {"expert": other})
    route_in[me] = route_out[me]

    own = weight_slice(0)
    for i in range(3):
        grad_own[i] = own[i]

    for t, ref in enumerate((out_ref, tgrad_ref)):
        copy(partner.at[t, 0], partner.at[t, 0], pc_send.at[t, 0], pc_recv.at[t, 0],
             {"expert": mate}).wait_recv()
        value = expand(0, t, 3, 4)
        wait_rows(has_up, chip + 1 == stages - 1, ret_in.at[t, chip], ret_recv.at[t, chip])
        wait_rows(has_down, chip - 1 == 0, ret_down.at[t], retd_recv.at[t])
        value += tn(up_hot.astype(BF16), ret_in[t, chip]) + tn(down_hot.astype(BF16), ret_down[t])
        ref[...] = value.astype(BF16)

    for off in range(1, groups):
        copy(route_out.at[0], route_in.at[0], route_send.at[off - 1], route_recv.at[off - 1],
             {"expert": mate}).wait_recv()
    route_ref[...] = route_in[...]
    for i, ref in enumerate((gg_ref, ug_ref, dg_ref)):
        value = grad_own[i]
        for off in range(1, ndp):
            copy(grad_recv.at[i, off - 1], grad_recv.at[i, off - 1], gr_send.at[i, off - 1],
                 gr_recv.at[i, off - 1], {"expert": mate}).wait_recv()
            value += grad_recv[i, off - 1].astype(F32)
        ref[...] = value.astype(BF16)
    for cond, args in pending:
        if cond is None:
            copy(*args).wait_send()
        else:
            pl.when(cond)(lambda args=args: copy(*args).wait_send())


def kernel_scratch(groups, ndp, cap, count, width, part, ff):
    stages = groups // CORES
    rows = groups * cap
    shapes = [
        ((2, 2, stages, count, width), BF16),
        ((2, count, width), BF16),
        ((groups, 8, count), F32),
        ((rows, width), BF16),
        ((rows, width), BF16),
        ((rows, width), BF16),
        ((rows, 128), F32),
        ((3, ndp, part, ff), BF16),
        ((2, rows, width), BF16),
        ((2, stages, cap, width), BF16),
        ((2, stages, count, width), BF16),
        ((2, count, width), BF16),
        ((2, stages, count, width), BF16),
        ((3, ndp - 1, part, ff), BF16),
        ((3, part, ff), F32),
        ((3, ndp - 1, part, ff), BF16),
        ((groups, 8, count), F32),
        ((groups, 8, count), F32),
    ]
    sems = [
        (2, stages, 3), (2, 2, stages), (groups - 1,), (groups - 1,), (3, ndp - 1), (3, ndp - 1),
        (2, stages), (2, stages), (2, stages), (2, stages), (2,), (groups - 1,), (groups - 1,),
        (3, ndp - 1), (3, ndp - 1),
    ]
    return shapes, sems


def scratch_bytes(shapes):
    total = 0
    for shape, dtype in shapes:
        size = jnp.dtype(dtype).itemsize
        for n in shape:
            size *= n
        total += size
    return total


def slot_capacity(count, top, experts):
    return max(2, (3 * count * top + 2 * experts - 1) // (2 * experts))


def line_body(groups, ndp, tokens, expert_ids, route_weights, w_gate, w_up, w_down, grad_out):
    count, width = tokens.shape
    _, part, ff = w_gate.shape
    top = expert_ids.shape[1]
    slots = slot_capacity(count, top, groups)
    cap = pad16(slots)
    edge = min(count, pad16(CORES * slots))
    meta, order = route_tables(expert_ids, route_weights, groups)
    shapes, sems = kernel_scratch(groups, ndp, cap, count, width, part, ff)
    vmem = pl.BlockSpec(memory_space=pltpu.VMEM)
    layer_out, token_grad, route, gate_g, up_g, down_g = pl.pallas_call(
        functools.partial(moe_kernel, groups, ndp, cap, edge),
        out_shape=(
            jax.ShapeDtypeStruct((count, width), BF16),
            jax.ShapeDtypeStruct((count, width), BF16),
            jax.ShapeDtypeStruct((groups, 8, count), F32),
            jax.ShapeDtypeStruct((part, ff), BF16),
            jax.ShapeDtypeStruct((part, ff), BF16),
            jax.ShapeDtypeStruct((part, ff), BF16),
        ),
        in_specs=[vmem] * 7,
        out_specs=(vmem,) * 6,
        scratch_shapes=[pltpu.VMEM(s, d) for s, d in shapes]
        + [pltpu.SemaphoreType.DMA(s) for s in sems],
        compiler_params=pltpu.CompilerParams(
            collective_id=0, has_side_effects=True, vmem_limit_bytes=VMEM_MAX
        ),
    )(tokens, grad_out, meta, order, w_gate[0], w_up[0], w_down[0])
    experts = lax.broadcasted_iota(jnp.int32, (groups, count, top), 0)
    mine = (expert_ids[None] == experts).astype(F32)
    route_grad = jnp.sum(mine * route[:, 0, :, None], axis=0)
    return layer_out, token_grad, route_grad, gate_g[None], up_g[None], down_g[None]


def pick_body(groups, ndp, *args):
    tokens, expert_ids, _, w_gate = args[:4]
    count, width = tokens.shape
    local, part, ff = w_gate.shape
    if local == 1 and groups % CORES == 0 and groups > CORES and ndp > 1:
        cap = pad16(slot_capacity(count, expert_ids.shape[1], groups))
        shapes, _ = kernel_scratch(groups, ndp, cap, count, width, part, ff)
        if scratch_bytes(shapes) < VMEM_MAX * 3 // 4:
            return line_body(groups, ndp, *args)
    return body(*args)


def solution(mesh):
    in_specs = (
        P(("dp", "expert"), None),
        P(("dp", "expert"), None),
        P(("dp", "expert"), None),
        P("expert", "dp", None),
        P("expert", "dp", None),
        P("expert", "dp", None),
        P(("dp", "expert"), None),
    )
    out_specs = (
        P(("dp", "expert"), None),
        P(("dp", "expert"), None),
        P(("dp", "expert"), None),
        P("expert", "dp", None),
        P("expert", "dp", None),
        P("expert", "dp", None),
    )
    step = functools.partial(pick_body, mesh.shape["expert"], mesh.shape["dp"])
    return jax.shard_map(step, mesh=mesh, in_specs=in_specs, out_specs=out_specs, check_vma=False)
```

```python
import functools

import jax
import jax.numpy as jnp
from jax import lax
from jax.experimental import pallas as pl
from jax.experimental.pallas import tpu as pltpu
from jax.sharding import PartitionSpec as P

BF16 = jnp.bfloat16
F32 = jnp.float32
CORES = 2
VMEM_MAX = 60 * 1024 * 1024


def slot_table(expert_ids, experts, capacity):
    flat = expert_ids.reshape(-1)
    count = flat.shape[0]
    same = flat[:, None] == flat[None, :]
    earlier = lax.broadcasted_iota(jnp.int32, (count, count), 0) > lax.broadcasted_iota(
        jnp.int32, (count, count), 1
    )
    rank = jnp.sum((same & earlier).astype(jnp.int32), axis=1)
    target = flat * capacity + rank
    columns = lax.broadcasted_iota(jnp.int32, (count, experts * capacity), 1)
    return (target[:, None] == columns).astype(jnp.bfloat16)


def contract_last(left, right):
    return lax.dot_general(
        left, right, (((1,), (1,)), ((), ())), preferred_element_type=jnp.float32
    )


def contract_first(left, right):
    return lax.dot_general(
        left, right, (((0,), (0,)), ((), ())), preferred_element_type=jnp.float32
    )


def expert_forward(rows, gate_w, up_w, down_w):
    gate = jnp.dot(rows, gate_w, preferred_element_type=jnp.float32)
    up = jnp.dot(rows, up_w, preferred_element_type=jnp.float32)
    sig = jax.nn.sigmoid(gate)
    hidden = (gate * sig * up).astype(jnp.bfloat16)
    expert_out = contract_last(hidden, down_w).astype(jnp.bfloat16)
    return (expert_out, (gate, up, sig, hidden))


def expert_backward(out_grad, saved, gate_w, up_w, down_w):
    gate, up, sig, hidden = saved
    hidden_grad = jnp.dot(out_grad, down_w, preferred_element_type=jnp.float32)
    gate_term = (hidden_grad * up * sig * (1.0 + gate * (1.0 - sig))).astype(jnp.bfloat16)
    up_term = (hidden_grad * gate * sig).astype(jnp.bfloat16)
    slot_grad = (contract_last(gate_term, gate_w) + contract_last(up_term, up_w)).astype(
        jnp.bfloat16
    )
    return (slot_grad, gate_term, up_term)


def weight_grads(rows, out_grad, gate_term, up_term, hidden):
    part_rows, part_grad = (
        lax.all_to_all(rows, "dp", split_axis=1, concat_axis=0, tiled=True),
        lax.all_to_all(out_grad, "dp", split_axis=1, concat_axis=0, tiled=True),
    )
    all_gate, all_up, all_hidden = (
        lax.all_gather(gate_term, "dp", axis=0, tiled=True),
        lax.all_gather(up_term, "dp", axis=0, tiled=True),
        lax.all_gather(hidden, "dp", axis=0, tiled=True),
    )
    down_g = contract_first(part_grad, all_hidden).astype(jnp.bfloat16)
    gate_g = contract_first(part_rows, all_gate).astype(jnp.bfloat16)
    up_g = contract_first(part_rows, all_up).astype(jnp.bfloat16)
    return (gate_g, up_g, down_g)


def body(tokens, expert_ids, route_weights, w_gate, w_up, w_down, grad_out):
    local = w_gate.shape[0]
    groups = lax.axis_size("expert")
    experts = local * groups
    count = tokens.shape[0]
    top = expert_ids.shape[1]
    width = tokens.shape[1]
    capacity = max(2, (3 * count * top + 2 * experts - 1) // (2 * experts))
    table = slot_table(expert_ids, experts, capacity)
    per_token = jnp.sum(table.reshape(count, top, experts * capacity), axis=1)
    send_rows = jnp.dot(per_token.T, tokens, preferred_element_type=jnp.float32)
    send_rows = send_rows.astype(jnp.bfloat16).reshape(experts, capacity, width)
    weighted = (route_weights[:, :, None] * grad_out.astype(jnp.float32)[:, None, :]).astype(
        jnp.bfloat16
    )
    send_grad = jnp.dot(
        table.T, weighted.reshape(count * top, width), preferred_element_type=jnp.float32
    )
    send_grad = send_grad.astype(jnp.bfloat16).reshape(experts, capacity, width)
    full_gate, full_up, full_down = (
        lax.all_gather(w_gate, "dp", axis=1, tiled=True),
        lax.all_gather(w_up, "dp", axis=1, tiled=True),
        lax.all_gather(w_down, "dp", axis=1, tiled=True),
    )
    received = lax.all_to_all(send_rows, "expert", split_axis=0, concat_axis=0, tiled=True)
    shaped = received.reshape(groups, local, capacity, width)
    saves = []
    inputs = []
    slot_expert = 0
    rows = shaped[:, slot_expert].reshape(groups * capacity, width)
    expert_out, saved = expert_forward(
        rows, full_gate[slot_expert], full_up[slot_expert], full_down[slot_expert]
    )
    outs = expert_out.reshape(groups, 1, capacity, width)
    saves.append(saved)
    inputs.append(rows)
    expert_outs, saves, inputs = (outs.reshape(experts, capacity, width), saves, inputs)
    back_out = lax.all_to_all(expert_outs, "expert", split_axis=0, concat_axis=0, tiled=True)
    received_grad = lax.all_to_all(send_grad, "expert", split_axis=0, concat_axis=0, tiled=True)
    shaped = received_grad.reshape(groups, local, capacity, width)
    slot_expert = 0
    out_grad = shaped[:, slot_expert].reshape(groups * capacity, width)
    slot_grad, gate_term, up_term = expert_backward(
        out_grad,
        saves[slot_expert],
        full_gate[slot_expert],
        full_up[slot_expert],
        full_down[slot_expert],
    )
    grads_in = slot_grad.reshape(groups, 1, capacity, width)
    gate_g, up_g, down_g = weight_grads(
        inputs[slot_expert], out_grad, gate_term, up_term, saves[slot_expert][3]
    )
    gate_list = [gate_g]
    up_list = [up_g]
    down_list = [down_g]
    slot_grads = grads_in.reshape(experts, capacity, width)
    gate_grad = jnp.stack(gate_list)
    up_grad = jnp.stack(up_list)
    down_grad = jnp.stack(down_list)
    back_grad = lax.all_to_all(slot_grads, "expert", split_axis=0, concat_axis=0, tiled=True)
    out_slots = jnp.dot(
        table, back_out.reshape(experts * capacity, width), preferred_element_type=jnp.float32
    )
    out_slots = out_slots.reshape(count, top, width)
    layer_out = jnp.sum(route_weights[:, :, None] * out_slots, axis=1).astype(jnp.bfloat16)
    route_grad = jnp.sum(grad_out.astype(jnp.float32)[:, None, :] * out_slots, axis=2)
    grad_slots = jnp.dot(
        table, back_grad.reshape(experts * capacity, width), preferred_element_type=jnp.float32
    )
    token_grad = jnp.sum(grad_slots.reshape(count, top, width), axis=1).astype(jnp.bfloat16)
    return (layer_out, token_grad, route_grad, gate_grad, up_grad, down_grad)


def pad16(n):
    return (n + 15) // 16 * 16


def prefix_count(member):
    t = member.shape[1]
    before = lax.broadcasted_iota(jnp.int32, (t, t), 0) < lax.broadcasted_iota(jnp.int32, (t, t), 1)
    return jnp.sum(member[:, :, None] * before.astype(F32)[None], axis=1)


def route_tables(expert_ids, route_weights, groups):
    count, top = expert_ids.shape
    stages = groups // CORES
    chip = lax.axis_index("expert") // CORES
    lanes = lax.broadcasted_iota(jnp.int32, (count,), 0)
    experts = lax.broadcasted_iota(jnp.int32, (groups, count), 0)
    member = jnp.zeros((groups, count), F32)
    weight = jnp.zeros((groups, count), F32)
    for k in range(top):
        hit = (expert_ids[:, k][None, :] == experts).astype(F32)
        member = member + hit
        weight = weight + hit * route_weights[:, k][None, :]
    slot = jnp.where(member > 0, prefix_count(member), -1.0)

    def position(first):
        key = jnp.where(first, lanes, lanes + count)
        return jnp.sum((key[:, None] < key[None, :]).astype(F32), axis=0)

    pos_up = position(jnp.any(expert_ids // CORES == stages - 1, axis=1))
    pos_down = position(jnp.any(expert_ids // CORES == 0, axis=1))
    dest = lax.broadcasted_iota(jnp.int32, (groups, 1), 0) // CORES
    pos = jnp.where(dest >= chip, pos_up[None, :], pos_down[None, :])
    pick = (pos[:, None, :] == lanes.astype(F32)[None, :, None]).astype(F32)
    slot_rows = jnp.sum(pick * slot[:, None, :], axis=2)
    weight_rows = jnp.sum(pick * weight[:, None, :], axis=2)
    swap = lambda a: a.reshape(stages, CORES, count)[:, ::-1].reshape(groups, count)
    zero = jnp.zeros_like(slot)
    meta = jnp.stack(
        [slot_rows, weight_rows, swap(slot_rows), slot, swap(slot), zero, zero, zero], axis=1
    )
    order = jnp.stack([pos_up, pos_down] + [jnp.zeros_like(pos_up)] * 6, axis=0)
    return meta, order


def one_hot(row, height):
    rows = lax.broadcasted_iota(jnp.int32, (height, row.shape[1]), 0).astype(F32)
    return (rows == row).astype(F32)


def choose(index, values):
    result = jnp.int32(values[0])
    for i in range(1, len(values)):
        result = jnp.where(index == i, jnp.int32(values[i]), result)
    return result


def visit_order(chip, stages):
    near = [s for d in range(stages) for s in ((chip - d, chip + d) if d else (chip,))]
    return [s for s in near if 0 <= s < stages]


def moe_kernel(
    groups, ndp, cap, edge,
    tok_ref, grad_ref, meta_ref, order_ref, wg_ref, wu_ref, wd_ref,
    out_ref, tgrad_ref, route_ref, gg_ref, ug_ref, dg_ref,
    blocks, own_down, metas, xr, gr, ogr, wr, wfull, y, partner, ret_in, ret_down, ret_out,
    grad_send, grad_own, grad_recv, route_out, route_in,
    in_send, in_recv, meta_send, meta_recv, w_send, w_recv, pc_send, pc_recv,
    ret_send, ret_recv, retd_recv, route_send, route_recv, gr_send, gr_recv,
):
    stages = groups // CORES
    count, width = tok_ref.shape
    part, ff = wg_ref.shape
    me = lax.axis_index("expert")
    dp = lax.axis_index("dp")
    chip, core = me // CORES, me % CORES
    mate = chip * CORES + (1 - core)
    at_edge = (chip == 0) | (chip == stages - 1)
    pending = []

    def copy(src, dst, ssem, rsem, where):
        return pltpu.make_async_remote_copy(
            src_ref=src, dst_ref=dst, send_sem=ssem, recv_sem=rsem,
            device_id=where, device_id_type=pl.DeviceIdType.MESH,
        )

    def send(cond, *args):
        if cond is None:
            copy(*args).start()
        else:
            pl.when(cond)(lambda: copy(*args).start())
        pending.append((cond, args))

    def send_rows(cond, short, src, dst, ssem, rsem, where):
        if edge == count:
            send(cond, src, dst, ssem, rsem, where)
            return
        full = jnp.logical_not(short)
        if cond is not None:
            short, full = cond & short, cond & full
        cut = pl.ds(0, edge)
        send(full, src, dst, ssem, rsem, where)
        send(short, src.at[cut], dst.at[cut], ssem, rsem, where)

    def wait_rows(cond, short, dst, sem):
        def one(c, ref):
            pl.when(c)(lambda: copy(ref, ref, sem, sem, {"expert": mate}).wait_recv())

        if edge == count:
            one(cond, dst)
            return
        one(cond & jnp.logical_not(short), dst)
        one(cond & short, dst.at[pl.ds(0, edge)])

    yes = chip >= 0
    if edge < count:
        rest = pl.ds(edge, count - edge)
        empty = jnp.zeros((count - edge, width), BF16)
        for t in range(2):
            for s in range(stages):
                blocks[0, t, s, rest] = empty
                blocks[1, t, s, rest] = empty
                ret_in[t, s, rest] = empty
            ret_down[t, rest] = empty
    for t in range(2):
        @pl.when(chip == stages - 1)
        def _():
            ret_in[t, chip] = jnp.zeros((count, width), BF16)

        @pl.when(chip == 0)
        def _():
            ret_down[t] = jnp.zeros((count, width), BF16)

    up_hot = one_hot(order_ref[0:1, :], count)
    down_hot = one_hot(order_ref[1:2, :], count)
    for t, ref in enumerate((tok_ref, grad_ref)):
        value = ref[...]
        blocks[0, t, chip] = jnp.dot(up_hot.astype(BF16), value, preferred_element_type=F32).astype(BF16)
        own_down[t] = jnp.dot(down_hot.astype(BF16), value, preferred_element_type=F32).astype(BF16)
    metas[me] = meta_ref[me]

    barrier = pltpu.get_barrier_semaphore()
    for off in range(1, groups):
        pl.semaphore_signal(barrier, inc=1, device_id={"expert": (me + off) % groups},
                            device_id_type=pl.DeviceIdType.MESH)
    for off in range(1, ndp):
        pl.semaphore_signal(barrier, inc=1, device_id={"dp": (dp + off) % ndp},
                            device_id_type=pl.DeviceIdType.MESH)
    pl.semaphore_wait(barrier, groups + ndp - 2)

    for off in range(1, groups):
        other = (me + off) % groups
        send(None, meta_ref.at[other], metas.at[me], meta_send.at[off - 1], meta_recv.at[off - 1],
             {"expert": other})
    has_up, has_down = chip < stages - 1, chip > 0
    up_dev, down_dev = {"expert": me + CORES}, {"expert": me - CORES}
    for t in range(2):
        send_rows(has_up, chip + 1 == stages - 1, blocks.at[0, t, chip], blocks.at[0, t, chip],
                  in_send.at[t, 0, 0], in_recv.at[0, t, chip], up_dev)
        send_rows(has_down, chip - 1 == 0, own_down.at[t], blocks.at[0, t, chip],
                  in_send.at[t, 0, 1], in_recv.at[0, t, chip], down_dev)
        send(None, blocks.at[0, t, chip], blocks.at[1, t, chip],
             in_send.at[t, 0, 2], in_recv.at[1, t, chip], {"expert": mate})
    for i, ref in enumerate((wg_ref, wu_ref, wd_ref)):
        for off in range(1, ndp):
            send(None, ref, wfull.at[i, dp], w_send.at[i, off - 1], w_recv.at[i, off - 1],
                 {"dp": (dp + off) % ndp})
        wfull[i, dp] = ref[...]
    for off in range(1, groups):
        copy(meta_ref.at[0], metas.at[0], meta_send.at[off - 1], meta_recv.at[off - 1],
             {"expert": mate}).wait_recv()

    table = [visit_order(z, stages) for z in range(stages)]
    source = [choose(chip, [table[z][q] for z in range(stages)]) for q in range(stages)]

    def compact(q, r):
        s = source[q]
        origin = s * CORES + (core if r == 0 else 1 - core)
        tile = metas[origin]
        hot = one_hot(tile[0:1, :], cap)
        scale = jnp.sum(hot * tile[1:2, :], axis=1, keepdims=True)
        hot = hot.astype(BF16)
        rows = pl.ds((q * 2 + r) * cap, cap)
        xr[rows, :] = jnp.dot(hot, blocks[r, 0, s], preferred_element_type=F32).astype(BF16)
        g = jnp.dot(hot, blocks[r, 1, s], preferred_element_type=F32)
        gr[rows, :] = g.astype(BF16)
        ogr[rows, :] = (scale * g).astype(BF16)
        wr[rows, :] = jnp.broadcast_to(scale, (cap, 128))

    compact(0, 0)
    for q in range(stages):
        s = source[q]
        if q:
            rising = s < chip
            nxt = jnp.where(rising, chip + 1, chip - 1)
            more = (nxt >= 0) & (nxt < stages)
            for t in range(2):
                wait_rows(yes, at_edge, blocks.at[0, t, s], in_recv.at[0, t, s])
                send_rows(more, (nxt == 0) | (nxt == stages - 1), blocks.at[0, t, s],
                          blocks.at[0, t, s], in_send.at[t, q, 0], in_recv.at[0, t, s],
                          {"expert": nxt * CORES + core})
                send_rows(None, at_edge, blocks.at[0, t, s], blocks.at[1, t, s],
                          in_send.at[t, q, 2], in_recv.at[1, t, s], {"expert": mate})
            compact(q, 0)
        for t in range(2):
            if q:
                wait_rows(yes, at_edge, blocks.at[1, t, s], in_recv.at[1, t, s])
            else:
                wait_rows(yes, chip < 0, blocks.at[1, t, s], in_recv.at[1, t, s])
        compact(q, 1)

    for i in range(3):
        for off in range(1, ndp):
            copy(wfull.at[i, 0], wfull.at[i, 0], w_send.at[i, 0], w_recv.at[i, off - 1],
                 {"expert": mate}).wait_recv()

    def nt(a, b):
        return lax.dot_general(a, b, (((1,), (1,)), ((), ())), preferred_element_type=F32)

    def tn(a, b):
        return lax.dot_general(a, b, (((0,), (0,)), ((), ())), preferred_element_type=F32)

    def cut(j):
        return pl.ds(j * part, part)

    total = xr.shape[0]
    gate = jnp.zeros((total, ff), F32)
    up = jnp.zeros((total, ff), F32)
    hg = jnp.zeros((total, ff), F32)
    for j in range(ndp):
        gate += jnp.dot(xr[:, cut(j)], wfull[0, j], preferred_element_type=F32)
        up += jnp.dot(xr[:, cut(j)], wfull[1, j], preferred_element_type=F32)
        hg += jnp.dot(ogr[:, cut(j)], wfull[2, j], preferred_element_type=F32)
    sig = jax.nn.sigmoid(gate)
    hidden = (gate * sig * up).astype(BF16)
    gt = (hg * up * sig * (1.0 + gate * (1.0 - sig))).astype(BF16)
    ut = (hg * gate * sig).astype(BF16)
    scale = wr[:, 0:1]
    dots = jnp.zeros((total, 1), F32)
    def to_mate(t):
        for q in reversed(range(stages)):
            send(None, y.at[t, pl.ds((q * 2 + 1) * cap, cap)], partner.at[t, q],
                 pc_send.at[t, q], pc_recv.at[t, q], {"expert": mate})

    for j in range(ndp):
        eo = nt(hidden, wfull[2, j]).astype(BF16).astype(F32)
        y[0, :, cut(j)] = (scale * eo).astype(BF16)
        dots += jnp.sum(gr[:, cut(j)].astype(F32) * eo, axis=1, keepdims=True)
    to_mate(0)
    for j in range(ndp):
        y[1, :, cut(j)] = (nt(gt, wfull[0, j]) + nt(ut, wfull[1, j])).astype(BF16)
    to_mate(1)

    both = jnp.concatenate([gt, ut], axis=1)

    def weight_slice(off):
        j = (dp + off) % ndp
        cols = pl.ds(pl.multiple_of(j * part, part), part)
        gu = tn(xr[:, cols], both)
        return gu[:, :ff], gu[:, ff:], tn(ogr[:, cols], hidden)

    def weight_part(off):
        for i, value in enumerate(weight_slice(off)):
            grad_send[i, off - 1] = value.astype(BF16)
        for i in range(3):
            send(None, grad_send.at[i, off - 1], grad_recv.at[i, off - 1], gr_send.at[i, off - 1],
                 gr_recv.at[i, off - 1], {"dp": (dp + off) % ndp})

    def expand(q, t, row_own, row_mate):
        tile = metas[source[q] * CORES + core]
        own = one_hot(tile[row_own:row_own + 1, :], cap).astype(BF16)
        other = one_hot(tile[row_mate:row_mate + 1, :], cap).astype(BF16)
        return tn(own, y[t, pl.ds(q * 2 * cap, cap), :]) + tn(other, partner[t, q])

    def give_back(q, ends):
        s = source[q]
        rising = s > chip
        nxt = jnp.where(rising, chip + 1, chip - 1)
        back = jnp.where(rising, chip - 1, chip + 1)
        where = {"expert": nxt * CORES + core}
        here = at_edge if ends else jnp.logical_not(at_edge)
        for t in range(2):
            pl.when(here)(lambda t=t: copy(
                partner.at[t, q], partner.at[t, q], pc_send.at[t, q], pc_recv.at[t, q],
                {"expert": mate}).wait_recv())
            if not ends:
                wait_rows(here, (back == 0) | (back == stages - 1), ret_in.at[t, s],
                          ret_recv.at[t, s])

            @pl.when(here)
            def _():
                value = expand(q, t, 0, 2)
                if not ends:
                    value = value + ret_in[t, s].astype(F32)
                ret_out[t, q] = value.astype(BF16)

            arrives = rising & (nxt == s)
            rows = pl.ds(0, edge) if ends else pl.ds(0, count)
            send(here & arrives, ret_out.at[t, q, rows], ret_down.at[t, rows], ret_send.at[t, q],
                 retd_recv.at[t], where)
            send(here & jnp.logical_not(arrives), ret_out.at[t, q, rows], ret_in.at[t, s, rows],
                 ret_send.at[t, q], ret_recv.at[t, s], where)

    for q in reversed(range(1, stages)):
        give_back(q, True)
    for off in range(1, ndp):
        weight_part(off)
    for q in reversed(range(1, stages)):
        give_back(q, False)

    for q in range(stages):
        for r in range(2):
            origin = source[q] * CORES + (core if r == 0 else 1 - core)
            hot = one_hot(metas[origin][3:4, :], cap)
            part_dots = dots[(q * 2 + r) * cap:(q * 2 + r + 1) * cap, :]
            line = jnp.sum(hot * part_dots, axis=0, keepdims=True)
            route_out[origin] = jnp.broadcast_to(line, (8, count))
    for off in range(1, groups):
        other = (me + off) % groups
        send(None, route_out.at[other], route_in.at[me], route_send.at[off - 1],
             route_recv.at[off - 1], {"expert": other})
    route_in[me] = route_out[me]

    own = weight_slice(0)
    for i in range(3):
        grad_own[i] = own[i]

    for t, ref in enumerate((out_ref, tgrad_ref)):
        copy(partner.at[t, 0], partner.at[t, 0], pc_send.at[t, 0], pc_recv.at[t, 0],
             {"expert": mate}).wait_recv()
        value = expand(0, t, 3, 4)
        wait_rows(has_up, chip + 1 == stages - 1, ret_in.at[t, chip], ret_recv.at[t, chip])
        wait_rows(has_down, chip - 1 == 0, ret_down.at[t], retd_recv.at[t])
        value += tn(up_hot.astype(BF16), ret_in[t, chip]) + tn(down_hot.astype(BF16), ret_down[t])
        ref[...] = value.astype(BF16)

    for off in range(1, groups):
        copy(route_out.at[0], route_in.at[0], route_send.at[off - 1], route_recv.at[off - 1],
             {"expert": mate}).wait_recv()
    route_ref[...] = route_in[...]
    for i, ref in enumerate((gg_ref, ug_ref, dg_ref)):
        value = grad_own[i]
        for off in range(1, ndp):
            copy(grad_recv.at[i, off - 1], grad_recv.at[i, off - 1], gr_send.at[i, off - 1],
                 gr_recv.at[i, off - 1], {"expert": mate}).wait_recv()
            value += grad_recv[i, off - 1].astype(F32)
        ref[...] = value.astype(BF16)
    for cond, args in pending:
        if cond is None:
            copy(*args).wait_send()
        else:
            pl.when(cond)(lambda args=args: copy(*args).wait_send())


def kernel_scratch(groups, ndp, cap, count, width, part, ff):
    stages = groups // CORES
    rows = groups * cap
    shapes = [
        ((2, 2, stages, count, width), BF16),
        ((2, count, width), BF16),
        ((groups, 8, count), F32),
        ((rows, width), BF16),
        ((rows, width), BF16),
        ((rows, width), BF16),
        ((rows, 128), F32),
        ((3, ndp, part, ff), BF16),
        ((2, rows, width), BF16),
        ((2, stages, cap, width), BF16),
        ((2, stages, count, width), BF16),
        ((2, count, width), BF16),
        ((2, stages, count, width), BF16),
        ((3, ndp - 1, part, ff), BF16),
        ((3, part, ff), F32),
        ((3, ndp - 1, part, ff), BF16),
        ((groups, 8, count), F32),
        ((groups, 8, count), F32),
    ]
    sems = [
        (2, stages, 3), (2, 2, stages), (groups - 1,), (groups - 1,), (3, ndp - 1), (3, ndp - 1),
        (2, stages), (2, stages), (2, stages), (2, stages), (2,), (groups - 1,), (groups - 1,),
        (3, ndp - 1), (3, ndp - 1),
    ]
    return shapes, sems


def scratch_bytes(shapes):
    total = 0
    for shape, dtype in shapes:
        size = jnp.dtype(dtype).itemsize
        for n in shape:
            size *= n
        total += size
    return total


def slot_capacity(count, top, experts):
    return max(2, (3 * count * top + 2 * experts - 1) // (2 * experts))


def line_body(groups, ndp, tokens, expert_ids, route_weights, w_gate, w_up, w_down, grad_out):
    count, width = tokens.shape
    _, part, ff = w_gate.shape
    top = expert_ids.shape[1]
    slots = slot_capacity(count, top, groups)
    cap = pad16(slots)
    edge = min(count, pad16(CORES * slots))
    meta, order = route_tables(expert_ids, route_weights, groups)
    shapes, sems = kernel_scratch(groups, ndp, cap, count, width, part, ff)
    vmem = pl.BlockSpec(memory_space=pltpu.VMEM)
    layer_out, token_grad, route, gate_g, up_g, down_g = pl.pallas_call(
        functools.partial(moe_kernel, groups, ndp, cap, edge),
        out_shape=(
            jax.ShapeDtypeStruct((count, width), BF16),
            jax.ShapeDtypeStruct((count, width), BF16),
            jax.ShapeDtypeStruct((groups, 8, count), F32),
            jax.ShapeDtypeStruct((part, ff), BF16),
            jax.ShapeDtypeStruct((part, ff), BF16),
            jax.ShapeDtypeStruct((part, ff), BF16),
        ),
        in_specs=[vmem] * 7,
        out_specs=(vmem,) * 6,
        scratch_shapes=[pltpu.VMEM(s, d) for s, d in shapes]
        + [pltpu.SemaphoreType.DMA(s) for s in sems],
        compiler_params=pltpu.CompilerParams(
            collective_id=0, has_side_effects=True, vmem_limit_bytes=VMEM_MAX
        ),
    )(tokens, grad_out, meta, order, w_gate[0], w_up[0], w_down[0])
    experts = lax.broadcasted_iota(jnp.int32, (groups, count, top), 0)
    mine = (expert_ids[None] == experts).astype(F32)
    route_grad = jnp.sum(mine * route[:, 0, :, None], axis=0)
    return layer_out, token_grad, route_grad, gate_g[None], up_g[None], down_g[None]


def pick_body(groups, ndp, *args):
    tokens, expert_ids, _, w_gate = args[:4]
    count, width = tokens.shape
    local, part, ff = w_gate.shape
    if local == 1 and groups % CORES == 0 and groups > CORES and ndp > 1:
        cap = pad16(slot_capacity(count, expert_ids.shape[1], groups))
        shapes, _ = kernel_scratch(groups, ndp, cap, count, width, part, ff)
        if scratch_bytes(shapes) < VMEM_MAX * 3 // 4:
            return line_body(groups, ndp, *args)
    return body(*args)


def solution(mesh):
    in_specs = (
        P(("dp", "expert"), None),
        P(("dp", "expert"), None),
        P(("dp", "expert"), None),
        P("expert", "dp", None),
        P("expert", "dp", None),
        P("expert", "dp", None),
        P(("dp", "expert"), None),
    )
    out_specs = (
        P(("dp", "expert"), None),
        P(("dp", "expert"), None),
        P(("dp", "expert"), None),
        P("expert", "dp", None),
        P("expert", "dp", None),
        P("expert", "dp", None),
    )
    step = functools.partial(pick_body, mesh.shape["expert"], mesh.shape["dp"])
    return jax.shard_map(step, mesh=mesh, in_specs=in_specs, out_specs=out_specs, check_vma=False)
```
